16 devices in a mesh: dp: 2 (over y, z), tp: 8 (over x, core).
Axes of the slice: x: 4, y: 2, z: 1, core: 2. Of those that a mesh axis runs over, the one named last changes fastest.
The devices are a block of a 4x4x8 slice.
Arguments:
- x_tokens: bfloat16 [32, 512, 3072], P('dp', 'tp'), parts along dimension 0
- e_time: float32 [32, 3, 3072], P('dp'), parts along dimension 0
- m_block: float32 [3, 3072], replicated
- w_q: bfloat16 [3072, 3072], P(None, 'tp')
- b_q: float32 [3072], P('tp')
- w_k: bfloat16 [3072, 3072], P(None, 'tp')
- b_k: float32 [3072], P('tp')
- w_v: bfloat16 [3072, 3072], P(None, 'tp')
- b_v: float32 [3072], P('tp')
- w_o: bfloat16 [3072, 3072], P('tp')
- b_o: float32 [3072], replicated
- g_q: float32 [3072], P('tp')
- g_k: float32 [3072], P('tp')
- positions: int32 [1024, 3], P('dp'), parts along dimension 0
- d_out: bfloat16 [32, 512, 3072], P('dp', 'tp'), parts along dimension 0
Outputs:
- output 1: bfloat16 [32, 512, 3072], P('dp', 'tp'), parts along dimension 0
- output 2: bfloat16 [32, 512, 3072], P('dp', 'tp'), parts along dimension 0
- output 3: float32 [32, 3, 3072], P('dp'), parts along dimension 0
- output 4: float32 [6, 3072], P('dp'), parts along dimension 0
- output 5: bfloat16 [6144, 3072], P('dp', 'tp'), parts along dimension 0
- output 6: bfloat16 [6144, 3072], P('dp', 'tp'), parts along dimension 0
- output 7: bfloat16 [6144, 3072], P('dp', 'tp'), parts along dimension 0
- output 8: bfloat16 [6144, 3072], P(('dp', 'tp')), parts along dimension 0
- output 9: float32 [6144], P(('dp', 'tp')), parts along dimension 0
- output 10: float32 [6144], P(('dp', 'tp')), parts along dimension 0
There are 2 independent parts. The reference program is written for one: setup_inputs(seed, part) draws one part's arguments, and reference() takes and returns one part's arrays. A program takes and returns all parts, laid end to end along the dimension named above; an argument that names none is the same for every part.
All inputs are finite; a program needn't handle non-finite values.
Results may differ from the reference program's by a relative error of at most 0.02.
Values are sent between devices in bfloat16 or wider.
A program may use at most 768 MiB of HBM per device.

```python
import jax
import jax.numpy as jnp
from jax import lax

NUM_BATCH = 16
SEQ_LEN = 512
NUM_HEADS = 24
HEAD_DIM = 128
MODEL_DIM = 3072
NUM_FRAMES = 21
NUM_ROWS = 45
NUM_COLS = 80

EPS_NORM = 1e-6
ROPE_BASE = 10000.0


def draw_positions(pos_key):
    coord_keys = jax.random.split(pos_key, 3)
    frame_ids = jax.random.randint(coord_keys[0], (SEQ_LEN,), 0, NUM_FRAMES)
    row_ids = jax.random.randint(coord_keys[1], (SEQ_LEN,), 0, NUM_ROWS)
    col_ids = jax.random.randint(coord_keys[2], (SEQ_LEN,), 0, NUM_COLS)
    grid_pos = jnp.stack([frame_ids, row_ids, col_ids], axis=1).astype(jnp.int32)
    corner_hi = jnp.array([NUM_FRAMES - 1, NUM_ROWS - 1, NUM_COLS - 1], dtype=jnp.int32)
    return grid_pos.at[0].set(corner_hi).at[1].set(jnp.zeros((3,), jnp.int32))


def setup_inputs(seed: int = 0, part: int = 0) -> dict:
    root_key = jax.random.key(seed)
    shared_keys = jax.random.split(root_key, 12)
    part_keys = jax.random.split(jax.random.fold_in(root_key, part), 4)
    fan_scale = MODEL_DIM ** -0.5
    head_ramp = 2.0 ** (2.0 * jnp.arange(NUM_HEADS, dtype=jnp.float32) / max(NUM_HEADS - 1, 1) - 1.0)
    col_scale = jnp.repeat(head_ramp, HEAD_DIM)
    sq_shape = (MODEL_DIM, MODEL_DIM)
    vec_shape = (MODEL_DIM,)
    tok_shape = (NUM_BATCH, SEQ_LEN, MODEL_DIM)
    return {
        'x_tokens': (0.5 * jax.random.normal(part_keys[0], tok_shape, jnp.float32)).astype(jnp.bfloat16),
        'e_time': 0.5 * jax.random.normal(part_keys[1], (NUM_BATCH, 3, MODEL_DIM), jnp.float32),
        'm_block': 0.5 * jax.random.normal(shared_keys[0], (3, MODEL_DIM), jnp.float32),
        'w_q': (jax.random.normal(shared_keys[1], sq_shape, jnp.float32) * fan_scale * col_scale).astype(jnp.bfloat16),
        'b_q': 0.5 * jax.random.normal(shared_keys[2], vec_shape, jnp.float32),
        'w_k': (jax.random.normal(shared_keys[3], sq_shape, jnp.float32) * fan_scale * col_scale).astype(jnp.bfloat16),
        'b_k': 0.5 * jax.random.normal(shared_keys[4], vec_shape, jnp.float32),
        'w_v': (jax.random.normal(shared_keys[5], sq_shape, jnp.float32) * (1.5 * fan_scale)).astype(jnp.bfloat16),
        'b_v': 0.5 * jax.random.normal(shared_keys[6], vec_shape, jnp.float32),
        'w_o': (jax.random.normal(shared_keys[7], sq_shape, jnp.float32) * fan_scale).astype(jnp.bfloat16),
        'b_o': 0.5 * jax.random.normal(shared_keys[8], vec_shape, jnp.float32),
        'g_q': jax.random.uniform(shared_keys[9], vec_shape, jnp.float32, 0.5, 1.5),
        'g_k': jax.random.uniform(shared_keys[10], vec_shape, jnp.float32, 0.5, 1.5),
        'positions': draw_positions(part_keys[3]),
        'd_out': jax.random.normal(part_keys[2], tok_shape, jnp.float32).astype(jnp.bfloat16),
    }


def rope_angles(positions):
    half_dim = HEAD_DIM // 2
    side_len = HEAD_DIM // 6
    first_len = half_dim - 2 * side_len
    pair_idx = jnp.arange(half_dim)
    section = (pair_idx >= first_len).astype(jnp.int32) + (pair_idx >= first_len + side_len).astype(jnp.int32)
    offset = jnp.where(section == 0, 0, jnp.where(section == 1, first_len, first_len + side_len))
    sec_width = jnp.where(section == 0, first_len, side_len)
    freq_vals = ROPE_BASE ** (-(pair_idx - offset).astype(jnp.float32) / sec_width.astype(jnp.float32))
    select = jnp.where(section[None, :] == jnp.arange(3)[:, None], freq_vals[None, :], 0.0)
    angles = jnp.sum(positions.astype(jnp.float32)[:, :, None] * select[None, :, :], axis=1)
    return jnp.cos(angles), jnp.sin(angles)


def rope_rotate(values, cos_part, sin_part):
    val_pairs = values.reshape(values.shape[:-1] + (values.shape[-1] // 2, 2))
    even_part = val_pairs[..., 0]
    odd_part = val_pairs[..., 1]
    rotated = jnp.stack([even_part * cos_part - odd_part * sin_part, even_part * sin_part + odd_part * cos_part], axis=-1)
    return rotated.reshape(values.shape)


def full_rms(values, gain):
    return values * lax.rsqrt(jnp.mean(values * values, axis=-1, keepdims=True) + EPS_NORM) * gain


def head_attention(operands):
    q_head, k_head, v_head = operands
    scores = jnp.einsum('bqd,bkd->bqk', q_head.astype(jnp.float32), k_head.astype(jnp.float32)) * HEAD_DIM ** -0.5
    attn_probs = jax.nn.softmax(scores, axis=-1).astype(jnp.bfloat16)
    return jnp.einsum('bqk,bkd->bqd', attn_probs.astype(jnp.float32), v_head.astype(jnp.float32)).astype(jnp.bfloat16)


def attention_block(x_tokens, e_time, m_block, w_q, b_q, w_k, b_k, w_v, b_v, w_o, b_o, g_q, g_k, cos_bcast, sin_bcast):
    head_shape = (NUM_BATCH, SEQ_LEN, NUM_HEADS, HEAD_DIM)
    mod_rows = m_block[None] + e_time
    shift_row = mod_rows[:, 0][:, None]
    scale_one = 1.0 + mod_rows[:, 1][:, None]
    gate_row = mod_rows[:, 2][:, None]
    x_float = x_tokens.astype(jnp.float32)
    centered = x_float - jnp.mean(x_float, axis=-1, keepdims=True)
    x_norm = centered * lax.rsqrt(jnp.mean(centered * centered, axis=-1, keepdims=True) + EPS_NORM)
    y_act = (x_norm * scale_one + shift_row).astype(jnp.bfloat16).reshape(NUM_BATCH * SEQ_LEN, MODEL_DIM)
    q_raw = jnp.dot(y_act, w_q, preferred_element_type=jnp.float32) + b_q
    k_raw = jnp.dot(y_act, w_k, preferred_element_type=jnp.float32) + b_k
    v_heads = (jnp.dot(y_act, w_v, preferred_element_type=jnp.float32) + b_v).astype(jnp.bfloat16).reshape(head_shape)
    q_rot = rope_rotate(full_rms(q_raw, g_q).reshape(head_shape), cos_bcast, sin_bcast).astype(jnp.bfloat16)
    k_rot = rope_rotate(full_rms(k_raw, g_k).reshape(head_shape), cos_bcast, sin_bcast).astype(jnp.bfloat16)
    o_heads = lax.map(jax.checkpoint(head_attention), (jnp.moveaxis(q_rot, 2, 0), jnp.moveaxis(k_rot, 2, 0), jnp.moveaxis(v_heads, 2, 0)))
    o_flat = jnp.moveaxis(o_heads, 0, 2).reshape(NUM_BATCH * SEQ_LEN, MODEL_DIM)
    proj_out = (jnp.dot(o_flat, w_o, preferred_element_type=jnp.float32) + b_o).reshape(NUM_BATCH, SEQ_LEN, MODEL_DIM)
    return (x_float + gate_row * proj_out).astype(jnp.bfloat16)


def reference(x_tokens, e_time, m_block, w_q, b_q, w_k, b_k, w_v, b_v, w_o, b_o, g_q, g_k, positions, d_out):
    cos_tab, sin_tab = rope_angles(positions)
    cos_bcast = cos_tab[None, :, None, :]
    sin_bcast = sin_tab[None, :, None, :]

    def block_fn(x_in, e_in, m_in, wq_in, wk_in, wv_in, wo_in, gq_in, gk_in):
        return attention_block(x_in, e_in, m_in, wq_in, b_q, wk_in, b_k, wv_in, b_v, wo_in, b_o, gq_in, gk_in, cos_bcast, sin_bcast)

    x_out, pull_back = jax.vjp(block_fn, x_tokens, e_time, m_block, w_q, w_k, w_v, w_o, g_q, g_k)
    d_x, d_e, d_m, d_wq, d_wk, d_wv, d_wo, d_gq, d_gk = pull_back(d_out)
    return (x_out, d_x, d_e, d_m, d_wq, d_wk, d_wv, d_wo, d_gq, d_gk)
```

```python
import functools

import jax
import jax.numpy as jnp
from jax import lax
from jax.experimental import pallas as pl
from jax.experimental.pallas import tpu as pltpu
from jax.sharding import PartitionSpec as P


HEAD_DIM = 128
EPS_NORM = 1e-6
ROPE_BASE = 10000.0
SCALE = HEAD_DIM ** -0.5
LOG2E = 1.4426950408889634
ROW_CONTRACT = (((0,), (0,)), ((), ()))
COL_CONTRACT = (((1,), (1,)), ((), ()))
MESH = pl.DeviceIdType.MESH
CHUNKS = 4
F32 = jnp.float32
BF16 = jnp.bfloat16


def rope_tables(positions):
    half_dim = HEAD_DIM // 2
    side_len = HEAD_DIM // 6
    first_len = half_dim - 2 * side_len
    lane = jnp.arange(HEAD_DIM)
    pair_idx = lane // 2
    section = (pair_idx >= first_len).astype(jnp.int32) + (pair_idx >= first_len + side_len).astype(jnp.int32)
    offset = jnp.where(section == 0, 0, jnp.where(section == 1, first_len, first_len + side_len))
    sec_width = jnp.where(section == 0, first_len, side_len)
    freq_vals = ROPE_BASE ** (-(pair_idx - offset).astype(F32) / sec_width.astype(F32))
    select = jnp.where(section[None, :] == jnp.arange(3)[:, None], freq_vals[None, :], 0.0)
    angles = jnp.sum(positions.astype(F32)[:, :, None] * select[None, :, :], axis=1)
    sign = jnp.where(lane % 2 == 0, -1.0, 1.0).astype(F32)
    return jnp.cos(angles), jnp.sin(angles) * sign[None, :]


def exchange_kernel(n, x_ref, out_ref, slots, send_sem, recv_sem):
    me = lax.axis_index("tp")
    barrier = pltpu.get_barrier_semaphore()
    for step in range(1, n):
        pl.semaphore_signal(barrier, inc=1, device_id={"tp": lax.rem(me + step, n)}, device_id_type=MESH)
    pl.semaphore_wait(barrier, n - 1)
    copies = []
    for step in range(1, n):
        copy = pltpu.make_async_remote_copy(
            src_ref=x_ref, dst_ref=slots.at[step - 1], send_sem=send_sem.at[step - 1], recv_sem=recv_sem.at[step - 1],
            device_id={"tp": lax.rem(me + step, n)}, device_id_type=MESH)
        copy.start()
        copies.append(copy)
    total = x_ref[...]
    for step in range(1, n):
        copies[step - 1].wait()
        total = total + slots[step - 1]
    out_ref[...] = total


def exchange_sum(x, n, cid):
    return pl.pallas_call(
        functools.partial(exchange_kernel, n),
        out_shape=jax.ShapeDtypeStruct(x.shape, x.dtype),
        in_specs=[pl.BlockSpec(memory_space=pltpu.VMEM)],
        out_specs=pl.BlockSpec(memory_space=pltpu.VMEM),
        scratch_shapes=[
            pltpu.VMEM((n - 1,) + x.shape, x.dtype),
            pltpu.SemaphoreType.DMA((n - 1,)),
            pltpu.SemaphoreType.DMA((n - 1,)),
        ],
        compiler_params=pltpu.CompilerParams(collective_id=cid, has_side_effects=True),
        cost_estimate=pl.CostEstimate(flops=4_000_000, bytes_accessed=200_000, transcendentals=0),
        name="exchange_sum",
    )(x)


def attn_kernel(heads, q0, q1, k0, k1, v0, v1, do0, do1, inv_ref, gq_ref, gk_ref, cos_ref, sin_ref,
                o0, o1, dq0, dq1, dk0, dk1, dv0, dv1, st_ref, dg_ref):
    half = q0.shape[1]
    seq = 2 * half
    cos_tab = cos_ref[...]
    sin_tab = sin_ref[...]
    lane = lax.broadcasted_iota(jnp.int32, (seq, HEAD_DIM), 1)
    even = (lane & 1) == 0

    def partner(x):
        return jnp.where(even, pltpu.roll(x, HEAD_DIM - 1, 1), pltpu.roll(x, 1, 1))

    def load(a, b, cols):
        return jnp.concatenate([a[0, :, cols], b[0, :, cols]], axis=0)

    def store(a, b, cols, x):
        a[0, :, cols] = x[:half]
        b[0, :, cols] = x[half:]

    inv_cols = jnp.transpose(inv_ref[0])
    inv_q = inv_cols[:, 0:1]
    inv_k = inv_cols[:, 1:2]

    @pl.when(pl.program_id(0) == 0)
    def _():
        dg_ref[...] = jnp.zeros_like(dg_ref)

    st_q = jnp.zeros((seq, 1), F32)
    st_k = jnp.zeros((seq, 1), F32)
    for h in range(heads):
        cols = slice(h * HEAD_DIM, (h + 1) * HEAD_DIM)
        gq = gq_ref[:, cols]
        gk = gk_ref[:, cols]
        q_hat = load(q0, q1, cols) * inv_q
        k_hat = load(k0, k1, cols) * inv_k
        qg = q_hat * gq
        kg = k_hat * gk
        q_rot = (qg * cos_tab + partner(qg) * sin_tab).astype(BF16)
        k_rot = (kg * cos_tab + partner(kg) * sin_tab).astype(BF16)
        v = load(v0, v1, cols)
        do = load(do0, do1, cols)
        s = lax.dot_general(q_rot, k_rot, COL_CONTRACT, preferred_element_type=F32)
        e = jnp.exp2((s - jnp.max(s, axis=-1, keepdims=True)) * (SCALE * LOG2E))
        p = e * (1.0 / jnp.sum(e, axis=-1, keepdims=True))
        pb = p.astype(BF16)
        store(o0, o1, cols, jnp.dot(pb, v, preferred_element_type=F32).astype(BF16))
        store(dv0, dv1, cols, lax.dot_general(pb, do, ROW_CONTRACT, preferred_element_type=F32).astype(BF16))
        dp = lax.dot_general(do, v, COL_CONTRACT, preferred_element_type=F32)
        t = dp * p
        ds = (t - p * jnp.sum(t, axis=-1, keepdims=True)).astype(BF16)
        dq = jnp.dot(ds, k_rot, preferred_element_type=F32) * SCALE
        dk = lax.dot_general(ds, q_rot, ROW_CONTRACT, preferred_element_type=F32) * SCALE
        dq = dq.astype(BF16).astype(F32)
        dk = dk.astype(BF16).astype(F32)
        dq_hat = dq * cos_tab - partner(dq) * sin_tab
        dk_hat = dk * cos_tab - partner(dk) * sin_tab
        dgq = dq_hat * q_hat
        dgk = dk_hat * k_hat
        dg_ref[0:1, cols] += jnp.sum(dgq, axis=0, keepdims=True)
        dg_ref[1:2, cols] += jnp.sum(dgk, axis=0, keepdims=True)
        st_q += jnp.sum(dgq * gq, axis=-1, keepdims=True)
        st_k += jnp.sum(dgk * gk, axis=-1, keepdims=True)
        store(dq0, dq1, cols, dq_hat * gq * inv_q)
        store(dk0, dk1, cols, dk_hat * gk * inv_k)
    stats = jnp.where(lane == 0, st_q, jnp.where(lane == 1, st_k, 0.0))
    st_ref[0] = jnp.transpose(stats)[:8, :]


def attention(q, k, v, do, inv_rows, g_q, g_k, cos_tab, sin_tab):
    batch, half, cols = q[0].shape
    seq = 2 * half
    heads = cols // HEAD_DIM
    big = pl.BlockSpec((1, half, cols), lambda b: (b, 0, 0))
    row8 = pl.BlockSpec((1, 8, seq), lambda b: (b, 0, 0))
    gain = pl.BlockSpec((1, cols), lambda b: (0, 0))
    tab = pl.BlockSpec((seq, HEAD_DIM), lambda b: (0, 0))
    sds = jax.ShapeDtypeStruct
    shape = (batch, half, cols)
    outs = pl.pallas_call(
        functools.partial(attn_kernel, heads),
        grid=(batch,),
        in_specs=[big] * 8 + [row8, gain, gain, tab, tab],
        out_specs=[big] * 8 + [row8, pl.BlockSpec((8, cols), lambda b: (0, 0))],
        out_shape=[sds(shape, BF16)] * 2 + [sds(shape, F32)] * 4 + [sds(shape, BF16)] * 2
        + [sds((batch, 8, seq), F32), sds((8, cols), F32)],
        compiler_params=pltpu.CompilerParams(dimension_semantics=("arbitrary",), vmem_limit_bytes=56 * 1024 * 1024),
        cost_estimate=pl.CostEstimate(flops=batch * heads * 24 * seq * seq * HEAD_DIM,
                                      bytes_accessed=batch * seq * cols * 24, transcendentals=batch * heads * seq * seq),
        name="attn_fwd_bwd",
    )(*q, *k, *v, *do, inv_rows, g_q[None], g_k[None], cos_tab, sin_tab)
    return outs[0:2], outs[2:4], outs[4:6], outs[6:8], outs[8], outs[9]


def dy_kernel(has_add, *refs):
    if has_add:
        aq, ak, q, k, dv, coef, wq, wk, wv, add, dq_out, dk_out, dy_out = refs
    else:
        aq, ak, q, k, dv, coef, wq, wk, wv, dq_out, dk_out, dy_out = refs
        add = None

    @pl.when(pl.program_id(0) == 0)
    def _():
        coef_cols = jnp.transpose(coef[...])
        dq_out[...] = (aq[...] - q[...] * coef_cols[:, 0:1]).astype(BF16)
        dk_out[...] = (ak[...] - k[...] * coef_cols[:, 1:2]).astype(BF16)

    total = lax.dot_general(dq_out[...], wq[...], COL_CONTRACT, preferred_element_type=F32)
    total += lax.dot_general(dk_out[...], wk[...], COL_CONTRACT, preferred_element_type=F32)
    total += lax.dot_general(dv[...], wv[...], COL_CONTRACT, preferred_element_type=F32)
    if has_add:
        total += add[...].astype(F32)
    dy_out[...] = total.astype(BF16)


def input_grad(aq, ak, q, k, dv, coef, w_q, w_k, w_v, add=None):
    rows, cols = aq.shape
    depth = w_q.shape[0]
    tile = next(t for t in (512, 384, 256, 128) if depth % t == 0)
    whole = pl.BlockSpec((rows, cols), lambda n: (0, 0))
    weight = pl.BlockSpec((tile, cols), lambda n: (n, 0))
    out_tile = pl.BlockSpec((rows, tile), lambda n: (0, n))
    extra = [] if add is None else [add]
    sds = jax.ShapeDtypeStruct
    return pl.pallas_call(
        functools.partial(dy_kernel, add is not None),
        grid=(depth // tile,),
        in_specs=[whole] * 5 + [pl.BlockSpec((8, rows), lambda n: (0, 0))] + [weight] * 3 + [out_tile] * len(extra),
        out_specs=[whole, whole, out_tile],
        out_shape=[sds((rows, cols), BF16), sds((rows, cols), BF16), sds((rows, depth), BF16)],
        compiler_params=pltpu.CompilerParams(dimension_semantics=("arbitrary",), vmem_limit_bytes=48 * 1024 * 1024),
        cost_estimate=pl.CostEstimate(flops=6 * rows * cols * depth, bytes_accessed=rows * (cols * 22 + depth * 2),
                                      transcendentals=0),
        name="input_grad",
    )(aq, ak, q, k, dv, coef, w_q, w_k, w_v, *extra)


def solution(mesh):
    tp_size = mesh.shape['tp']

    def device_step(x_loc, e_loc, m_block, w_q, b_q, w_k, b_k, w_v, b_v, w_o, b_o, g_q, g_k, pos_part, dy_loc):
        batch_size, seq_loc, model_dim = x_loc.shape
        seq_len = seq_loc * tp_size
        cols = w_q.shape[1]
        chunks = CHUNKS
        nb = batch_size // chunks
        half = seq_len // 2
        hrows = nb * half
        parity = lax.axis_index('tp') % 2
        rings = [list(range(0, tp_size, 2)), list(range(1, tp_size, 2))]
        swap = [(i, i ^ 1) for i in range(tp_size)]
        pos_pairs = pos_part.reshape(tp_size // 2, 2, seq_loc, 3)
        pos_pairs = jnp.where(parity == 0, pos_pairs, pos_pairs[:, ::-1])
        cos_tab, sin_tab = rope_tables(pos_pairs.transpose(1, 0, 2, 3).reshape(seq_len, 3))

        mod_rows = m_block[None] + e_loc
        shift_row = mod_rows[:, 0][:, None]
        scale_one = 1.0 + mod_rows[:, 1][:, None]
        gate_row = mod_rows[:, 2][:, None]

        def part(a, i):
            return a[i * nb:(i + 1) * nb]

        def gather(a):
            own = lax.all_gather(a, 'tp', axis=1, tiled=True, axis_index_groups=rings)
            return own, lax.ppermute(own, 'tp', swap)

        def reduce_scatter(a):
            return lax.psum_scatter(a, 'tp', scatter_dimension=1, tiled=True, axis_index_groups=rings)

        def canonical(own, other, axis):
            first = jnp.where(parity == 0, own, other)
            return jnp.concatenate([first, jnp.where(parity == 0, other, own)], axis=axis)

        def norm_parts(x_part):
            x_float = x_part.astype(F32)
            centered = x_float - jnp.mean(x_float, axis=-1, keepdims=True)
            inv_std = lax.rsqrt(jnp.mean(centered * centered, axis=-1, keepdims=True) + EPS_NORM)
            return x_float, centered * inv_std, inv_std

        y_full, d_proj = [], []
        for i in range(chunks):
            x_norm = norm_parts(part(x_loc, i))[1]
            y_full.append(gather((x_norm * part(scale_one, i) + part(shift_row, i)).astype(BF16)))
            d_proj.append(gather((part(dy_loc, i).astype(F32) * part(gate_row, i)).astype(BF16)))

        x_outs, d_xs, d_mods, o_parts, dqs, dks, dvs, dgs = [], [], [], [], [], [], [], []
        projs, d_ys, ys, dps = [], [], [], []
        for i in range(chunks):
            y = [a.reshape(hrows, model_dim) for a in y_full[i]]
            dp = [a.reshape(hrows, model_dim) for a in d_proj[i]]
            q_raw = [jnp.dot(a, w_q, preferred_element_type=F32) + b_q for a in y]
            k_raw = [jnp.dot(a, w_k, preferred_element_type=F32) + b_k for a in y]
            v = [(jnp.dot(a, w_v, preferred_element_type=F32) + b_v).astype(BF16) for a in y]
            sq = [jnp.stack([jnp.sum(a * a, axis=-1), jnp.sum(b * b, axis=-1)]) for a, b in zip(q_raw, k_raw)]
            sq = [a.reshape(2 * nb, half) for a in sq]
            sq = exchange_sum(canonical(sq[0], sq[1], 1), tp_size, 2 * i)
            inv = lax.rsqrt(sq / model_dim + EPS_NORM)
            inv = canonical(inv[:, :half], inv[:, half:], 1).reshape(2, nb, seq_len)
            inv_rows = jnp.pad(inv.transpose(1, 0, 2), ((0, 0), (0, 6), (0, 0)))
            do = [lax.dot_general(a, w_o, COL_CONTRACT, preferred_element_type=F32).astype(BF16) for a in dp]

            def to_heads(pair):
                return [a.reshape(nb, half, cols) for a in pair]

            def to_rows(pair):
                return [a.reshape(hrows, cols) for a in pair]

            o, dq_s, dk_s, dv, st, dg = attention(to_heads(q_raw), to_heads(k_raw), to_heads(v), to_heads(do),
                                                  inv_rows, g_q, g_k, cos_tab, sin_tab)
            o, dq_s, dk_s, dv = to_rows(o), to_rows(dq_s), to_rows(dk_s), to_rows(dv)
            away = lax.ppermute(jnp.dot(o[1], w_o, preferred_element_type=F32).astype(BF16), 'tp', swap)
            part_sum = (jnp.dot(o[0], w_o, preferred_element_type=F32) + away.astype(F32)).astype(BF16)
            projs.append(reduce_scatter(part_sum.reshape(nb, half, model_dim)))
            st = st[:, :2].transpose(1, 0, 2).reshape(2 * nb, seq_len)
            st = exchange_sum(canonical(st[:, :half], st[:, half:], 1), tp_size, 2 * i + 1)
            st = canonical(st[:, :half], st[:, half:], 1).reshape(2, nb, 2, half)
            coef = st * (inv * inv / model_dim).reshape(2, nb, 2, half)
            coef = jnp.pad(coef.transpose(2, 0, 1, 3).reshape(2, 2, hrows), ((0, 0), (0, 6), (0, 0)))
            dq_b, dk_b, away = input_grad(dq_s[1], dk_s[1], q_raw[1], k_raw[1], dv[1], coef[1], w_q, w_k, w_v)
            away = lax.ppermute(away, 'tp', swap)
            dq_a, dk_a, dy_part = input_grad(dq_s[0], dk_s[0], q_raw[0], k_raw[0], dv[0], coef[0], w_q, w_k, w_v, away)
            d_ys.append(reduce_scatter(dy_part.reshape(nb, half, model_dim)))
            ys += y
            dps += dp
            o_parts += o
            dqs += [dq_a, dq_b]
            dks += [dk_a, dk_b]
            dvs += dv
            dgs.append(dg)

        def weight_grad(lefts, rights):
            total = None
            for a, b in zip(lefts, rights):
                term = lax.dot_general(a, b, ROW_CONTRACT, preferred_element_type=F32)
                total = term if total is None else total + term
            return total.astype(BF16)

        d_wo = weight_grad(o_parts, dps)
        d_wq = weight_grad(ys, dqs)
        d_wk = weight_grad(ys, dks)
        d_wv = weight_grad(ys, dvs)

        for i in range(chunks):
            proj, x_part, dy_part = lax.optimization_barrier((projs[i], part(x_loc, i), part(dy_loc, i)))
            proj = proj.astype(F32) + b_o
            x_outs.append((x_part.astype(F32) + part(gate_row, i) * proj).astype(BF16))
            d_gate = jnp.sum(dy_part.astype(F32) * proj, axis=1)
            d_y, x_part, dy_part = lax.optimization_barrier((d_ys[i], part(x_loc, i), part(dy_loc, i)))
            dy_float = dy_part.astype(F32)
            _, x_norm, inv_std = norm_parts(x_part)
            d_y = d_y.astype(F32)
            d_mods.append(jnp.stack([jnp.sum(d_y, axis=1), jnp.sum(d_y * x_norm, axis=1), d_gate], axis=1))
            d_norm = d_y * part(scale_one, i)
            d_xs.append((dy_float + inv_std * (d_norm - jnp.mean(d_norm, axis=-1, keepdims=True)
                                               - x_norm * jnp.mean(d_norm * x_norm, axis=-1, keepdims=True))).astype(BF16))
        d_mod = lax.psum(jnp.concatenate(d_mods, axis=0), 'tp')
        dg = functools.reduce(jnp.add, dgs)
        return (jnp.concatenate(x_outs, axis=0), jnp.concatenate(d_xs, axis=0), d_mod, jnp.sum(d_mod, axis=0),
                d_wq, d_wk, d_wv, d_wo, dg[0], dg[1])

    in_specs = (P('dp', 'tp', None), P('dp', None, None), P(None, None), P(None, 'tp'), P('tp'), P(None, 'tp'), P('tp'),
                P(None, 'tp'), P('tp'), P('tp', None), P(None), P('tp'), P('tp'), P('dp', None), P('dp', 'tp', None))
    out_specs = (P('dp', 'tp', None), P('dp', 'tp', None), P('dp', None, None), P('dp', None), P('dp', 'tp'), P('dp', 'tp'),
                 P('dp', 'tp'), P(('dp', 'tp'), None), P(('dp', 'tp')), P(('dp', 'tp')))
    return jax.shard_map(device_step, mesh=mesh, in_specs=in_specs, out_specs=out_specs, check_vma=False)
```
